32 devices in a mesh: section: 2 (over y), expert: 16 (over z, x, core).
Axes of the slice: x: 2, y: 2, z: 4, core: 2. Of those that a mesh axis runs over, the one named last changes fastest.
Arguments:
- tokens: bfloat16 [2, 2048, 2048], P(None, 'expert'), may hold values from -6 to 6
- norm_gain: float32 [2, 2048], P('section'), may hold values from 0.1 to 1.9
- w_gate: bfloat16 [2, 16, 2048, 704], P('section', 'expert'), may hold values from -0.125 to 0.125
- w_up: bfloat16 [2, 16, 2048, 704], P('section', 'expert'), may hold values from -0.125 to 0.125
- w_down: bfloat16 [2, 16, 704, 2048], P('section', 'expert'), may hold values from -0.21875 to 0.21875
- expert_ids: int32 [2, 2, 2048, 6], P('section', None, 'expert'), may hold values from 0 to 15, all different within a row; in each aligned block of 128 rows (0 to 127, 128 to 255, ..., all dimensions but the last counted through in order) at most 49 rows name the same one
- route_weight: float32 [2, 2, 2048, 6], P('section', None, 'expert'), may hold values from 0.1 to 1
Outputs:
- stream: bfloat16 [2, 2, 2048, 2048], P('section', None, 'expert')
The draws below stay inside these ranges and needn't reach their ends.
Inputs may be any that keep to these rules, and one draw needn't show every extreme that they name: `expert_ids`: A token names 6 different experts. In each aligned block of 128 tokens (the tokens of one device in one layer and micro-batch) no expert is named by more than 49 tokens, a bound that some block reaches.
All inputs are finite; a program needn't handle non-finite values.
Results may differ from the reference program's by a relative error of at most 0.025.
Values may be sent and summed in bfloat16 or wider, within the bound.
A program may use at most 128 MiB of HBM per device.

```python
import math
import jax
import jax.numpy as jnp
import numpy as np
from jax import lax

D = 2048
HID = 704
TOP = 6
MB = 2
TOK_DEV = 128
EXPERTS = 16
LAYERS = 2
TOKENS = 2048
CAP = 49
N_EXPERT = 16


def block_scale(own_key, extent, pieces, least, high):
    loudness, own = 1.0, jax.random.fold_in(own_key, 6)
    for position, shards_of in pieces:
        draws = jnp.exp(jax.random.uniform(jax.random.fold_in(own, position), (shards_of,), jnp.float32, least / len(pieces), high / len(pieces)))
        loudness = loudness * jnp.repeat(draws, extent[position] // shards_of).reshape([-1 if axis == position else 1 for axis in range(len(extent))])
    return loudness


def deal_out(key, own, number, rows, amount, top, most, skew):
    order = jax.random.permutation(key, amount)
    heavy_load, common = load_shares(amount, rows * top, most, skew, True), load_shares(amount, rows * top, most, skew, False)
    places = jnp.arange(amount)

    def named(tallies, offset_by):
        used = int((tallies > 0).sum())
        fixed = max(1, used // 4)
        moved = fixed + (places - fixed + offset_by * (used - fixed)) % max(1, amount - fixed)
        return jnp.zeros((amount,), jnp.int32).at[order[jnp.where(places < fixed, places, moved)]].set(jnp.asarray(tallies, jnp.int32))

    tallies = jnp.where(number % 4 == 0, named(heavy_load, number // 4), named(common, number - number // 4 - 1))
    mixed = jax.random.permutation(jax.random.fold_in(own, 3), amount)
    donor, sink = mixed[0:amount // 2 * 2:2], mixed[1:amount // 2 * 2:2]
    room = jnp.minimum(tallies[donor] - 1, most - tallies[sink]) // 2
    room = jnp.where((donor == order[0]) | (sink == order[0]) | (tallies[sink] == 0), 0, jnp.maximum(room, 0))
    moved = jax.random.randint(jax.random.fold_in(own, 4), (amount // 2,), 0, 1 << 20) % (room + 1)
    tallies = tallies.at[donor].add(-moved).at[sink].add(moved)
    members = jnp.searchsorted(jnp.cumsum(tallies), jnp.arange(rows * top), side="right").astype(jnp.int32)
    listing = members.reshape(top, rows).T
    listing = listing[jax.random.permutation(jax.random.fold_in(own, 1), rows)]
    offset_by = jax.random.randint(jax.random.fold_in(own, 2), (rows, 1), 0, top)
    return jnp.take_along_axis(listing, (jnp.arange(top)[None, :] + offset_by) % top, axis=1)


def load_shares(amount, total, reach, slope, full):
    weights = [(1 << 20) // math.isqrt(grade ** slope) + 1 for grade in range(1, amount + 1)]
    largest = reach if full else min(reach, max(-(-total // amount), total * weights[0] // sum(weights)))
    least = 1 if total - largest >= amount - 1 else 0
    counts, rest = [largest] + [least] * (amount - 1), total - largest - least * (amount - 1)
    while rest > 0:
        free = [i for i in range(1, amount) if counts[i] < largest] or [i for i in range(1, amount) if counts[i] < reach]
        whole, budget = sum([weights[i] for i in free]), rest
        for i in free:
            more = min(reach - counts[i], max(1, budget * weights[i] // whole), rest)
            counts[i] = counts[i] + more
            rest = rest - more
    return np.array(counts)


def scatter_about(stream_key, shape, spread, bound, cuts=(), held_as=jnp.bfloat16):
    result = jax.random.normal(stream_key, shape, jnp.float32) * spread
    if len(cuts) > 0:
        result = block_scale(stream_key, shape, cuts, -0.22, 0.18) * result
    return jnp.clip(result, min=-bound, max=bound).astype(held_as)


def setup_inputs(seed: int = 0) -> dict:
    seeds = jax.random.split(jax.random.key(seed), 8)
    tokens = scatter_about(seeds[0], (MB, TOKENS, D), 1.0, 6.0, ((1, 16),))
    norm_gain = jnp.clip(1.0 + 0.18 * jax.random.normal(seeds[1], (LAYERS, D), jnp.float32), 0.1, 1.9)
    w_gate = scatter_about(seeds[2], (LAYERS, EXPERTS, D, HID), D ** -0.5, 0.125, ((0, 2), (1, 16)))
    w_up = scatter_about(seeds[3], (LAYERS, EXPERTS, D, HID), D ** -0.5, 0.125, ((0, 2), (1, 16)))
    w_down = scatter_about(seeds[4], (LAYERS, EXPERTS, HID, D), HID ** -0.5, 0.21875, ((0, 2), (1, 16)))
    expert_ids_keys = jax.random.split(jax.random.fold_in(seeds[5], 1), LAYERS * MB * TOKENS // TOK_DEV)
    expert_ids_turns = jax.random.permutation(jax.random.fold_in(seeds[5], 3), LAYERS * MB * TOKENS // TOK_DEV)
    expert_ids = jax.vmap(lambda own, number: deal_out(jax.random.fold_in(seeds[5], 2), own, number, TOK_DEV, EXPERTS, TOP, CAP, 0))(expert_ids_keys, expert_ids_turns).reshape((LAYERS, MB, TOKENS, TOP))
    route_weight = jnp.clip(jnp.exp(math.log(1.0) - 2.3025851 * jax.random.uniform(seeds[6], (LAYERS, MB, TOKENS, TOP), jnp.float32) ** block_scale(seeds[6], (LAYERS, MB, TOKENS, TOP), ((0, 2), (2, 16)), -0.2, 0.2)), 0.1, 1.0)
    return {"tokens": tokens, "norm_gain": norm_gain, "w_gate": w_gate, "w_up": w_up, "w_down": w_down, "expert_ids": expert_ids, "route_weight": route_weight}


epsilon = 1e-06

def expert_mlp(operands):
    inputs, gate_matrix, up_matrix, down_matrix = operands
    gate_proj = jnp.dot(inputs, gate_matrix, preferred_element_type=jnp.float32)
    upward = jnp.dot(inputs, up_matrix, preferred_element_type=jnp.float32)
    hidden = (jax.nn.silu(gate_proj) * upward).astype(jnp.bfloat16)
    return jnp.dot(hidden, down_matrix, preferred_element_type=jnp.float32).astype(jnp.bfloat16)

def layer_apply(residual, norm_scale, gate_all, up_all, down_all, route_ids, weights):
    values = residual.astype(jnp.float32)
    inverse_rms = lax.rsqrt(lax.optimization_barrier(jnp.mean(values * values, axis=-1, keepdims=True)) + epsilon)
    normed = (values * inverse_rms * norm_scale).astype(jnp.bfloat16)
    grouped = route_ids.reshape(N_EXPERT, TOK_DEV * TOP)
    onehot = (grouped[:, :, None] == jnp.arange(EXPERTS, dtype=jnp.int32)[None, None, :]).astype(jnp.int32)
    slot_index = lax.optimization_barrier(jnp.sum((jnp.cumsum(onehot, axis=1) - 1) * onehot, axis=-1))
    target = (jnp.arange(N_EXPERT, dtype=jnp.int32)[:, None] * CAP + slot_index).reshape(-1).astype(jnp.int32)
    chosen = route_ids.reshape(-1).astype(jnp.int32)
    owners = (jnp.arange(TOKENS * TOP, dtype=jnp.int32) // TOP).astype(jnp.int32)
    buffers = jnp.zeros((EXPERTS, N_EXPERT * CAP, D), jnp.bfloat16).at[chosen, target].set(normed[owners])
    results = lax.map(expert_mlp, (buffers, gate_all, up_all, down_all))
    picked = results[chosen, target].reshape(TOKENS, TOP, D).astype(jnp.float32)
    combined = values + lax.optimization_barrier(jnp.sum(weights[:, :, None] * picked, axis=1))
    return combined.astype(jnp.bfloat16)

def reference(tokens, norm_gain, w_gate, w_up, w_down, expert_ids, route_weight):
    states = [tokens[index] for index in range(MB)]
    layer_rows = []
    for layer in range(LAYERS):
        micro_rows = []
        for index in range(MB):
            states[index] = layer_apply(states[index], norm_gain[layer], w_gate[layer], w_up[layer], w_down[layer], expert_ids[layer, index], route_weight[layer, index])
            micro_rows.append(states[index])
        layer_rows.append(jnp.stack(micro_rows))
    return jnp.stack(layer_rows)
```

```python
import functools

import jax
import jax.numpy as jnp
from jax import lax
from jax.experimental import pallas as pl
from jax.experimental.pallas import tpu as pltpu
from jax.sharding import PartitionSpec as P

epsilon = 1e-06
MESH = pl.DeviceIdType.MESH
CORES = 2
COLS = 2
SUBS = 2
PIECES = 2 * SUBS


def ring_place():
    count = lax.axis_size("expert")
    chips = count // CORES
    depth = chips // COLS
    me = lax.axis_index("expert")
    lane = me % CORES
    chip = me // CORES
    col = chip % COLS
    high = chip // COLS
    spot = high + col * (2 * depth - 1 - 2 * high)

    def device(spot_of, lane_of):
        spot_of = (spot_of + 2 * chips) % chips
        half = spot_of // depth
        along = spot_of % depth
        level = along + half * (depth - 1 - 2 * along)
        return (level * COLS + half) * CORES + lane_of

    return count, chips, me, lane, spot, device


def gather_kernel(x_ref, out_ref, send_sem, recv_sem, sib_send, sib_recv, own_sem):
    count, chips, me, lane, spot, device = ring_place()
    towards = (device(spot + 1, lane), device(spot - 1, lane))
    sibling = device(spot, 1 - lane)
    rows = x_ref.shape[0] // PIECES

    barrier = pltpu.get_barrier_semaphore()
    for other in (*towards, sibling):
        pl.semaphore_signal(barrier, inc=1, device_id={"expert": other}, device_id_type=MESH)
    pl.semaphore_wait(barrier, 3)

    def piece_copy(source, origin, step, piece, target, sends, recvs):
        window = pl.ds(piece * rows, rows)
        src = x_ref.at[window] if source is None else out_ref.at[source, window]
        return pltpu.make_async_remote_copy(
            src_ref=src,
            dst_ref=out_ref.at[origin, window],
            send_sem=sends.at[step, piece],
            recv_sem=recvs.at[step, piece],
            device_id={"expert": target},
            device_id_type=MESH,
        )

    order = [(way * SUBS + sub, way) for sub in range(SUBS) for way in range(2)]
    for piece, way in order:
        piece_copy(None, me, 0, piece, towards[way], send_sem, recv_sem).start()
    own = pltpu.make_async_copy(x_ref, out_ref.at[me], own_sem)
    own.start()
    for piece, way in order:
        piece_copy(None, me, 0, piece, sibling, sib_send, sib_recv).start()

    def arrive(step, forward):
        for piece, way in order:
            origin = device(spot - step if way == 0 else spot + step, lane)
            piece_copy(origin, origin, step - 1, piece, towards[way], send_sem, recv_sem).wait_recv()
            if forward:
                piece_copy(origin, origin, step, piece, towards[way], send_sem, recv_sem).start()
            piece_copy(origin, origin, step, piece, sibling, sib_send, sib_recv).start()

    @pl.loop(1, chips - 1)
    def _(step):
        arrive(step, True)

    arrive(chips - 1, False)
    own.wait()

    @pl.loop(0, chips)
    def _(step):
        for piece, way in order:
            mine = device(spot - step if way == 0 else spot + step, lane)
            theirs = device(spot - step if way == 0 else spot + step, 1 - lane)
            piece_copy(mine, mine, step, piece, sibling, sib_send, sib_recv).wait_send()
            piece_copy(theirs, theirs, step, piece, sibling, sib_send, sib_recv).wait_recv()

    @pl.loop(0, chips - 1)
    def _(step):
        for piece, way in order:
            piece_copy(me, me, step, piece, towards[way], send_sem, recv_sem).wait_send()


def ring_gather(block):
    count = lax.axis_size("expert")
    chips = count // CORES
    return pl.pallas_call(
        gather_kernel,
        out_shape=jax.ShapeDtypeStruct((count,) + block.shape, block.dtype),
        in_specs=[pl.BlockSpec(memory_space=pltpu.VMEM)],
        out_specs=pl.BlockSpec(memory_space=pltpu.VMEM),
        scratch_shapes=[
            pltpu.SemaphoreType.DMA((chips, PIECES)),
            pltpu.SemaphoreType.DMA((chips, PIECES)),
            pltpu.SemaphoreType.DMA((chips, PIECES)),
            pltpu.SemaphoreType.DMA((chips, PIECES)),
            pltpu.SemaphoreType.DMA,
        ],
        compiler_params=pltpu.CompilerParams(collective_id=0, has_side_effects=True),
        name="ring_gather",
    )(block)


def scatter_kernel(
    part_ref, res_ref, out_ref, next_ref, held, slots,
    send_sem, recv_sem, sib_send, sib_recv, next_send, next_recv,
):
    count, chips, me, lane, spot, device = ring_place()
    sections = lax.axis_size("section")
    section = lax.axis_index("section")
    after, before = (section + 1) % sections, (section + sections - 1) % sections
    towards = (device(spot + 1, lane), device(spot - 1, lane))
    sibling = device(spot, 1 - lane)
    rows = res_ref.shape[0] // PIECES

    barrier = pltpu.get_barrier_semaphore()
    for other in (*towards, sibling):
        pl.semaphore_signal(barrier, inc=1, device_id={"expert": other}, device_id_type=MESH)
    pl.semaphore_signal(barrier, inc=1, device_id={"section": before}, device_id_type=MESH)
    pl.semaphore_wait(barrier, 4)

    order = [(way * SUBS + sub, way) for sub in range(SUBS) for way in range(2)]

    def goal(step, way):
        return spot - 1 - step if way == 0 else spot + 1 + step

    def sib_copy(step, piece, way):
        window = pl.ds(piece * rows, rows)
        return pltpu.make_async_remote_copy(
            src_ref=part_ref.at[device(goal(step, way), 1 - lane), window],
            dst_ref=held.at[step, window],
            send_sem=sib_send.at[step, piece],
            recv_sem=sib_recv.at[step, piece],
            device_id={"expert": sibling},
            device_id_type=MESH,
        )

    def ring_copy(src_ref, step, piece, way):
        window = pl.ds(piece * rows, rows)
        return pltpu.make_async_remote_copy(
            src_ref=src_ref.at[step if src_ref is held else step - 1, window],
            dst_ref=slots.at[step, window],
            send_sem=send_sem.at[step, piece],
            recv_sem=recv_sem.at[step, piece],
            device_id={"expert": towards[way]},
            device_id_type=MESH,
        )

    def next_copy(piece):
        window = pl.ds(piece * rows, rows)
        return pltpu.make_async_remote_copy(
            src_ref=out_ref.at[window],
            dst_ref=next_ref.at[window],
            send_sem=next_send.at[piece],
            recv_sem=next_recv.at[piece],
            device_id={"section": after},
            device_id_type=MESH,
        )

    @pl.loop(0, chips)
    def _(step):
        for piece, way in order:
            sib_copy(step, piece, way).start()

    def local(step, piece, way):
        window = pl.ds(piece * rows, rows)
        sib_copy(step, piece, way).wait_recv()
        mine = part_ref[device(goal(step, way), lane), window]
        return mine.astype(jnp.float32) + held[step, window].astype(jnp.float32)

    for piece, way in order:
        window = pl.ds(piece * rows, rows)
        held[0, window] = local(0, piece, way).astype(jnp.bfloat16)
        ring_copy(held, 0, piece, way).start()

    @pl.loop(1, chips - 1)
    def _(step):
        for piece, way in order:
            window = pl.ds(piece * rows, rows)
            own = local(step, piece, way)
            ring_copy(held, step - 1, piece, way).wait_recv()
            slots[step - 1, window] = (own + slots[step - 1, window].astype(jnp.float32)).astype(jnp.bfloat16)
            ring_copy(slots, step, piece, way).start()

    for piece, way in order:
        window = pl.ds(piece * rows, rows)
        own = local(chips - 1, piece, way) + res_ref[window].astype(jnp.float32)
        ring_copy(held, chips - 2, piece, way).wait_recv()
        out_ref[window] = (own + slots[chips - 2, window].astype(jnp.float32)).astype(jnp.bfloat16)
        next_copy(piece).start()

    @pl.loop(0, chips)
    def _(step):
        for piece, way in order:
            sib_copy(step, piece, way).wait_send()

    @pl.loop(0, chips - 1)
    def _(step):
        for piece, way in order:
            ring_copy(held, step, piece, way).wait_send()

    for piece, way in order:
        next_copy(piece).wait()


def ring_scatter(parts, residual):
    count = lax.axis_size("expert")
    chips = count // CORES
    vmem = pl.BlockSpec(memory_space=pltpu.VMEM)
    shape = jax.ShapeDtypeStruct(residual.shape, residual.dtype)
    return pl.pallas_call(
        scatter_kernel,
        out_shape=(shape, shape),
        in_specs=[vmem, vmem],
        out_specs=(vmem, vmem),
        scratch_shapes=[
            pltpu.VMEM((chips,) + residual.shape, residual.dtype),
            pltpu.VMEM((chips,) + residual.shape, residual.dtype),
            pltpu.SemaphoreType.DMA((chips, PIECES)),
            pltpu.SemaphoreType.DMA((chips, PIECES)),
            pltpu.SemaphoreType.DMA((chips, PIECES)),
            pltpu.SemaphoreType.DMA((chips, PIECES)),
            pltpu.SemaphoreType.DMA((PIECES,)),
            pltpu.SemaphoreType.DMA((PIECES,)),
        ],
        compiler_params=pltpu.CompilerParams(collective_id=1, has_side_effects=True),
        name="ring_scatter",
    )(parts, residual)


def rms_normed(row_block, norm_scale):
    values = row_block.astype(jnp.float32)
    inverse_rms = lax.rsqrt(jnp.mean(values * values, axis=-1, keepdims=True) + epsilon)
    return (values * inverse_rms * norm_scale).astype(jnp.bfloat16)


def per_device(tokens, norm_gain, w_gate, w_up, w_down, expert_ids, route_weight):
    groups = lax.axis_size("expert")
    sections = lax.axis_size("section")
    position = lax.axis_index("section")
    expert = lax.axis_index("expert")
    micro_count, tok_rows, model_width = tokens.shape
    fanout = expert_ids.shape[-1]
    capacity = -(-(tok_rows * fanout // groups + 1) // 8) * 8
    norm_scale = norm_gain[0]
    gate_matrix = w_gate[0, 0]
    up_matrix = w_up[0, 0]
    down_matrix = w_down[0, 0]

    all_ids = lax.all_gather(expert_ids[0], "expert", axis=0)
    all_weights = lax.all_gather(route_weight[0], "expert", axis=0)
    named = all_ids == expert
    chosen = named.any(axis=-1)
    share = jnp.sum(jnp.where(named, all_weights, 0.0), axis=-1)
    slot = jnp.cumsum(chosen.astype(jnp.int32), axis=-1) - 1
    slot = jnp.where(chosen, slot, -1)
    picks = slot[:, :, None, :] == jnp.arange(capacity, dtype=jnp.int32)[None, None, :, None]
    row_share = jnp.sum(jnp.where(picks, share[:, :, None, :], 0.0), axis=-1)
    selector = picks.astype(jnp.bfloat16)

    def layer_step(residual, which):
        gathered = ring_gather(rms_normed(residual, norm_scale))
        select = lax.dynamic_index_in_dim(selector, which, 1, keepdims=False)
        weight = lax.dynamic_index_in_dim(row_share, which, 1, keepdims=False)
        rows = jnp.einsum(
            "bct,btd->bcd", select, gathered, preferred_element_type=jnp.float32
        ).astype(jnp.bfloat16).reshape(groups * capacity, model_width)
        gate_proj = jnp.dot(rows, gate_matrix, preferred_element_type=jnp.float32)
        upward = jnp.dot(rows, up_matrix, preferred_element_type=jnp.float32)
        hidden = (jax.nn.silu(gate_proj) * upward).astype(jnp.bfloat16)
        result = jnp.dot(hidden, down_matrix, preferred_element_type=jnp.float32)
        result = (result * weight.reshape(-1)[:, None]).astype(jnp.bfloat16)
        parts = jnp.einsum(
            "bct,bcd->btd", select, result.reshape(groups, capacity, model_width),
            preferred_element_type=jnp.float32,
        ).astype(jnp.bfloat16)
        return ring_scatter(parts, residual)

    incoming = jnp.zeros((tok_rows, model_width), jnp.bfloat16)
    stream = jnp.zeros((micro_count, tok_rows, model_width), jnp.bfloat16)
    for moment in range(micro_count + sections - 1):
        micro_idx = moment - position
        active = jnp.logical_and(micro_idx >= 0, micro_idx < micro_count)
        which = jnp.clip(micro_idx, 0, micro_count - 1)
        entering = tokens[min(moment, micro_count - 1)]
        residual = jnp.where(position == 0, entering, incoming)
        result, incoming = layer_step(residual, which)
        stored = lax.dynamic_update_index_in_dim(stream, result, which, 0)
        stream = jnp.where(active, stored, stream)
    return stream[None]


def solution(mesh):
    return jax.shard_map(
        per_device,
        mesh=mesh,
        in_specs=(
            P(None, "expert", None),
            P("section", None),
            P("section", "expert", None, None),
            P("section", "expert", None, None),
            P("section", "expert", None, None),
            P("section", None, "expert", None),
            P("section", None, "expert", None),
        ),
        out_specs=P("section", None, "expert", None),
        check_vma=False,
    )
```

```python
import functools

import jax
import jax.numpy as jnp
from jax import lax
from jax.experimental import pallas as pl
from jax.experimental.pallas import tpu as pltpu
from jax.sharding import PartitionSpec as P

epsilon = 1e-06
MESH = pl.DeviceIdType.MESH
CORES = 2
COLS = 2
SUBS = 2
PIECES = 2 * SUBS


def ring_place():
    count = lax.axis_size("expert")
    chips = count // CORES
    depth = chips // COLS
    me = lax.axis_index("expert")
    lane = me % CORES
    chip = me // CORES
    col = chip % COLS
    high = chip // COLS
    spot = high + col * (2 * depth - 1 - 2 * high)

    def device(spot_of, lane_of):
        spot_of = (spot_of + 2 * chips) % chips
        half = spot_of // depth
        along = spot_of % depth
        level = along + half * (depth - 1 - 2 * along)
        return (level * COLS + half) * CORES + lane_of

    return count, chips, me, lane, spot, device


def gather_kernel(x_ref, out_ref, send_sem, recv_sem, sib_send, sib_recv, own_sem):
    count, chips, me, lane, spot, device = ring_place()
    towards = (device(spot + 1, lane), device(spot - 1, lane))
    sibling = device(spot, 1 - lane)
    rows = x_ref.shape[0] // PIECES

    barrier = pltpu.get_barrier_semaphore()
    for other in (*towards, sibling):
        pl.semaphore_signal(barrier, inc=1, device_id={"expert": other}, device_id_type=MESH)
    pl.semaphore_wait(barrier, 3)

    def piece_copy(source, origin, step, piece, target, sends, recvs):
        window = pl.ds(piece * rows, rows)
        src = x_ref.at[window] if source is None else out_ref.at[source, window]
        return pltpu.make_async_remote_copy(
            src_ref=src,
            dst_ref=out_ref.at[origin, window],
            send_sem=sends.at[step, piece],
            recv_sem=recvs.at[step, piece],
            device_id={"expert": target},
            device_id_type=MESH,
        )

    order = [(way * SUBS + sub, way) for sub in range(SUBS) for way in range(2)]
    for piece, way in order:
        piece_copy(None, me, 0, piece, towards[way], send_sem, recv_sem).start()
    own = pltpu.make_async_copy(x_ref, out_ref.at[me], own_sem)
    own.start()
    for piece, way in order:
        piece_copy(None, me, 0, piece, sibling, sib_send, sib_recv).start()

    def arrive(step, forward):
        for piece, way in order:
            origin = device(spot - step if way == 0 else spot + step, lane)
            piece_copy(origin, origin, step - 1, piece, towards[way], send_sem, recv_sem).wait_recv()
            if forward:
                piece_copy(origin, origin, step, piece, towards[way], send_sem, recv_sem).start()
            piece_copy(origin, origin, step, piece, sibling, sib_send, sib_recv).start()

    @pl.loop(1, chips - 1)
    def _(step):
        arrive(step, True)

    arrive(chips - 1, False)
    own.wait()

    @pl.loop(0, chips)
    def _(step):
        for piece, way in order:
            mine = device(spot - step if way == 0 else spot + step, lane)
            theirs = device(spot - step if way == 0 else spot + step, 1 - lane)
            piece_copy(mine, mine, step, piece, sibling, sib_send, sib_recv).wait_send()
            piece_copy(theirs, theirs, step, piece, sibling, sib_send, sib_recv).wait_recv()

    @pl.loop(0, chips - 1)
    def _(step):
        for piece, way in order:
            piece_copy(me, me, step, piece, towards[way], send_sem, recv_sem).wait_send()


def ring_gather(block):
    count = lax.axis_size("expert")
    chips = count // CORES
    return pl.pallas_call(
        gather_kernel,
        out_shape=jax.ShapeDtypeStruct((count,) + block.shape, block.dtype),
        in_specs=[pl.BlockSpec(memory_space=pltpu.VMEM)],
        out_specs=pl.BlockSpec(memory_space=pltpu.VMEM),
        scratch_shapes=[
            pltpu.SemaphoreType.DMA((chips, PIECES)),
            pltpu.SemaphoreType.DMA((chips, PIECES)),
            pltpu.SemaphoreType.DMA((chips, PIECES)),
            pltpu.SemaphoreType.DMA((chips, PIECES)),
            pltpu.SemaphoreType.DMA,
        ],
        compiler_params=pltpu.CompilerParams(collective_id=0, has_side_effects=True),
        name="ring_gather",
    )(block)


def exchange_kernel(x_ref, out_ref, send_sem, recv_sem, own_sem):
    count = lax.axis_size("expert")
    me = lax.axis_index("expert")
    barrier = pltpu.get_barrier_semaphore()

    @pl.loop(1, count)
    def _(shift):
        other = (me + shift) % count
        pl.semaphore_signal(barrier, inc=1, device_id={"expert": other}, device_id_type=MESH)

    pl.semaphore_wait(barrier, count - 1)

    def copy(shift):
        return pltpu.make_async_remote_copy(
            src_ref=x_ref,
            dst_ref=out_ref.at[me],
            send_sem=send_sem.at[shift],
            recv_sem=recv_sem.at[shift],
            device_id={"expert": (me + shift) % count},
            device_id_type=MESH,
        )

    @pl.loop(1, count)
    def _(shift):
        copy(shift).start()

    own = pltpu.make_async_copy(x_ref, out_ref.at[me], own_sem)
    own.start()
    own.wait()

    @pl.loop(1, count)
    def _(shift):
        copy(shift).wait_send()
        source = (me + count - shift) % count
        pltpu.make_async_remote_copy(
            src_ref=x_ref,
            dst_ref=out_ref.at[source],
            send_sem=send_sem.at[shift],
            recv_sem=recv_sem.at[shift],
            device_id={"expert": source},
            device_id_type=MESH,
        ).wait_recv()


def exchange(block):
    count = lax.axis_size("expert")
    return pl.pallas_call(
        exchange_kernel,
        out_shape=jax.ShapeDtypeStruct((count,) + block.shape, block.dtype),
        in_specs=[pl.BlockSpec(memory_space=pltpu.VMEM)],
        out_specs=pl.BlockSpec(memory_space=pltpu.VMEM),
        scratch_shapes=[
            pltpu.SemaphoreType.DMA((count,)),
            pltpu.SemaphoreType.DMA((count,)),
            pltpu.SemaphoreType.DMA,
        ],
        compiler_params=pltpu.CompilerParams(collective_id=2, has_side_effects=True),
        name="exchange",
    )(block)


def scatter_kernel(handoff, part_ref, res_ref, out_ref, *rest):
    if handoff:
        next_ref, held, slots, send_sem, recv_sem, sib_send, sib_recv, next_send, next_recv = rest
    else:
        held, slots, send_sem, recv_sem, sib_send, sib_recv = rest
    count, chips, me, lane, spot, device = ring_place()
    sections = lax.axis_size("section")
    section = lax.axis_index("section")
    after, before = (section + 1) % sections, (section + sections - 1) % sections
    towards = (device(spot + 1, lane), device(spot - 1, lane))
    sibling = device(spot, 1 - lane)
    rows = res_ref.shape[0] // PIECES

    barrier = pltpu.get_barrier_semaphore()
    for other in (*towards, sibling):
        pl.semaphore_signal(barrier, inc=1, device_id={"expert": other}, device_id_type=MESH)
    if handoff:
        pl.semaphore_signal(barrier, inc=1, device_id={"section": before}, device_id_type=MESH)
    pl.semaphore_wait(barrier, 4 if handoff else 3)

    order = [(way * SUBS + sub, way) for sub in range(SUBS) for way in range(2)]

    def goal(step, way):
        return spot - 1 - step if way == 0 else spot + 1 + step

    def sib_copy(step, piece, way):
        window = pl.ds(piece * rows, rows)
        return pltpu.make_async_remote_copy(
            src_ref=part_ref.at[device(goal(step, way), 1 - lane), window],
            dst_ref=held.at[step, window],
            send_sem=sib_send.at[step, piece],
            recv_sem=sib_recv.at[step, piece],
            device_id={"expert": sibling},
            device_id_type=MESH,
        )

    def ring_copy(src_ref, step, piece, way):
        window = pl.ds(piece * rows, rows)
        return pltpu.make_async_remote_copy(
            src_ref=src_ref.at[step if src_ref is held else step - 1, window],
            dst_ref=slots.at[step, window],
            send_sem=send_sem.at[step, piece],
            recv_sem=recv_sem.at[step, piece],
            device_id={"expert": towards[way]},
            device_id_type=MESH,
        )

    def next_copy(piece):
        window = pl.ds(piece * rows, rows)
        return pltpu.make_async_remote_copy(
            src_ref=out_ref.at[window],
            dst_ref=next_ref.at[window],
            send_sem=next_send.at[piece],
            recv_sem=next_recv.at[piece],
            device_id={"section": after},
            device_id_type=MESH,
        )

    @pl.loop(0, chips)
    def _(step):
        for piece, way in order:
            sib_copy(step, piece, way).start()

    def local(step, piece, way):
        window = pl.ds(piece * rows, rows)
        sib_copy(step, piece, way).wait_recv()
        mine = part_ref[device(goal(step, way), lane), window]
        return mine.astype(jnp.float32) + held[step, window].astype(jnp.float32)

    for piece, way in order:
        window = pl.ds(piece * rows, rows)
        held[0, window] = local(0, piece, way).astype(jnp.bfloat16)
        ring_copy(held, 0, piece, way).start()

    @pl.loop(1, chips - 1)
    def _(step):
        for piece, way in order:
            window = pl.ds(piece * rows, rows)
            own = local(step, piece, way)
            ring_copy(held, step - 1, piece, way).wait_recv()
            slots[step - 1, window] = (own + slots[step - 1, window].astype(jnp.float32)).astype(jnp.bfloat16)
            ring_copy(slots, step, piece, way).start()

    for piece, way in order:
        window = pl.ds(piece * rows, rows)
        own = local(chips - 1, piece, way) + res_ref[window].astype(jnp.float32)
        ring_copy(held, chips - 2, piece, way).wait_recv()
        out_ref[window] = (own + slots[chips - 2, window].astype(jnp.float32)).astype(jnp.bfloat16)
        if handoff:
            next_copy(piece).start()

    @pl.loop(0, chips)
    def _(step):
        for piece, way in order:
            sib_copy(step, piece, way).wait_send()

    @pl.loop(0, chips - 1)
    def _(step):
        for piece, way in order:
            ring_copy(held, step, piece, way).wait_send()

    if handoff:
        for piece, way in order:
            next_copy(piece).wait()


def ring_scatter(parts, residual, handoff):
    count = lax.axis_size("expert")
    chips = count // CORES
    vmem = pl.BlockSpec(memory_space=pltpu.VMEM)
    shape = jax.ShapeDtypeStruct(residual.shape, residual.dtype)
    return pl.pallas_call(
        functools.partial(scatter_kernel, handoff),
        out_shape=(shape, shape) if handoff else (shape,),
        in_specs=[vmem, vmem],
        out_specs=(vmem, vmem) if handoff else (vmem,),
        scratch_shapes=[
            pltpu.VMEM((chips,) + residual.shape, residual.dtype),
            pltpu.VMEM((chips,) + residual.shape, residual.dtype),
            pltpu.SemaphoreType.DMA((chips, PIECES)),
            pltpu.SemaphoreType.DMA((chips, PIECES)),
            pltpu.SemaphoreType.DMA((chips, PIECES)),
            pltpu.SemaphoreType.DMA((chips, PIECES)),
        ]
        + [pltpu.SemaphoreType.DMA((PIECES,))] * (2 if handoff else 0),
        compiler_params=pltpu.CompilerParams(
            collective_id=1 if handoff else 3, has_side_effects=True
        ),
        name="ring_scatter" if handoff else "ring_scatter_last",
    )(parts, residual)


def rms_normed(row_block, norm_scale):
    values = row_block.astype(jnp.float32)
    inverse_rms = lax.rsqrt(jnp.mean(values * values, axis=-1, keepdims=True) + epsilon)
    return (values * inverse_rms * norm_scale).astype(jnp.bfloat16)


def per_device(tokens, norm_gain, w_gate, w_up, w_down, expert_ids, route_weight):
    groups = lax.axis_size("expert")
    sections = lax.axis_size("section")
    position = lax.axis_index("section")
    expert = lax.axis_index("expert")
    micro_count, tok_rows, model_width = tokens.shape
    fanout = expert_ids.shape[-1]
    capacity = -(-(tok_rows * fanout // groups + 1) // 8) * 8
    norm_scale = norm_gain[0]
    gate_matrix = w_gate[0, 0]
    up_matrix = w_up[0, 0]
    down_matrix = w_down[0, 0]

    packed = jnp.stack([expert_ids[0].astype(jnp.float32), route_weight[0]])
    packed = packed.transpose(0, 1, 3, 2).reshape(2 * micro_count * fanout, tok_rows)
    routing = exchange(packed).reshape(groups, 2, micro_count, fanout, tok_rows)
    named = routing[:, 0] == expert.astype(jnp.float32)
    chosen = named.any(axis=2)
    share = jnp.sum(jnp.where(named, routing[:, 1], 0.0), axis=2)
    slot = jnp.cumsum(chosen.astype(jnp.int32), axis=-1) - 1
    slot = jnp.where(chosen, slot, -1)
    picks = slot[:, :, None, :] == jnp.arange(capacity, dtype=jnp.int32)[None, None, :, None]
    row_share = jnp.sum(jnp.where(picks, share[:, :, None, :], 0.0), axis=-1)
    selector = picks.astype(jnp.bfloat16)

    def layer_step(residual, which, handoff):
        gathered = ring_gather(rms_normed(residual, norm_scale))
        select = lax.dynamic_index_in_dim(selector, which, 1, keepdims=False)
        weight = lax.dynamic_index_in_dim(row_share, which, 1, keepdims=False)
        rows = jnp.einsum(
            "bct,btd->bcd", select, gathered, preferred_element_type=jnp.float32
        ).astype(jnp.bfloat16).reshape(groups * capacity, model_width)
        gate_proj = jnp.dot(rows, gate_matrix, preferred_element_type=jnp.float32)
        upward = jnp.dot(rows, up_matrix, preferred_element_type=jnp.float32)
        hidden = (jax.nn.silu(gate_proj) * upward).astype(jnp.bfloat16)
        result = jnp.dot(hidden, down_matrix, preferred_element_type=jnp.float32)
        result = (result * weight.reshape(-1)[:, None]).astype(jnp.bfloat16)
        parts = jnp.einsum(
            "bct,bcd->btd", select, result.reshape(groups, capacity, model_width),
            preferred_element_type=jnp.float32,
        ).astype(jnp.bfloat16)
        return ring_scatter(parts, residual, handoff)

    incoming = jnp.zeros((tok_rows, model_width), jnp.bfloat16)
    moments = micro_count + sections - 1
    results = []
    for moment in range(moments):
        which = jnp.clip(moment - position, 0, micro_count - 1)
        entering = tokens[min(moment, micro_count - 1)]
        residual = jnp.where(position == 0, entering, incoming)
        result, *handed = layer_step(residual, which, moment < moments - 1)
        incoming = handed[0] if handed else incoming
        results.append(result)
    stream = []
    for micro in range(micro_count):
        kept = results[micro]
        for section in range(1, sections):
            kept = jnp.where(position == section, results[micro + section], kept)
        stream.append(kept)
    return jnp.stack(stream)[None]


def solution(mesh):
    return jax.shard_map(
        per_device,
        mesh=mesh,
        in_specs=(
            P(None, "expert", None),
            P("section", None),
            P("section", "expert", None, None),
            P("section", "expert", None, None),
            P("section", "expert", None, None),
            P("section", None, "expert", None),
            P("section", None, "expert", None),
        ),
        out_specs=P("section", None, "expert", None),
        check_vma=False,
    )
```
